32 devices in a mesh: zg: 2 (over x), xy: 16 (over z, y, core).
Axes of the slice: x: 2, y: 2, z: 4, core: 2. Of those that a mesh axis runs over, the one named last changes fastest.
Arguments:
- charges: float32 [65536], P(('zg', 'xy')), may hold values from -12 to 12
- cells: int32 [8, 65536], P(None, ('zg', 'xy')), may hold values from 0 to 3145727
- splines: float32 [8, 65536], P(None, ('zg', 'xy')), may hold values from 0.05 to 1
- counts: int32 [32], P(('zg', 'xy')), may hold values from 1024 to 2048, as said below
- green: bfloat16 [512, 4, 384, 384], P(('zg', 'xy')), may hold values from -0.3125 to 0.3125
Outputs:
- potential: float32 [384, 512, 512], P(('zg', 'xy'))
The draws below stay inside these ranges and needn't reach their ends.
Inputs may be any that keep to these rules, and one draw needn't show every extreme that they name: `counts`: some device has all 2048 slots live in every draw.
All inputs are finite; a program needn't handle non-finite values.
Results may differ from the reference program's by a relative error of at most 0.0041.
Values may be sent and summed in bfloat16 or wider, within the bound.
A program may use at most 128 MiB of HBM per device.

```python
import jax
import jax.numpy as jnp
from jax import lax

NX = 512
NY = 512
NZ = 384
KYB = 4
SPREAD = 8
PART_DEV = 2048
ZDEV = 12
PARTICLES = 65536
N_ZG = 2
N_XY = 16
DEVICES = 32


def draw_counts(key, part):
    first = jax.random.fold_in(key, 11)
    second = jax.random.fold_in(key, 23)
    values = jax.random.randint(first, (DEVICES,), PART_DEV // 2, PART_DEV + 1, dtype=jnp.int32)
    chosen = jax.random.randint(second, (), 0, DEVICES, dtype=jnp.int32)
    places = jnp.arange(DEVICES, dtype=jnp.int32)
    return jnp.where(places == chosen, PART_DEV, values).astype(jnp.int32)


def plant(entries, stream_key, low, top_value):
    index_at = [jax.random.randint(jax.random.fold_in(stream_key, axis), (), 0, length) for axis, length in enumerate(entries.shape)]
    longest = entries.shape.index(max(entries.shape))
    next_to = index_at[:longest] + [(index_at[longest] + 1) % entries.shape[longest]] + index_at[longest + 1:]
    return entries.at[tuple(index_at)].set(low).at[tuple(next_to)].set(top_value)


def steps_of(stream_key, shape, split, smallest, high):
    def one(axis_at, blocks):
        heights = jax.random.uniform(jax.random.fold_in(jax.random.fold_in(stream_key, 6), axis_at), (blocks,), jnp.float32, smallest / len(split), high / len(split))
        return jnp.repeat(jnp.exp(heights), shape[axis_at] // blocks).reshape((-1,) + (1,) * (len(shape) - axis_at - 1))

    level = one(*split[0])
    for cut in split[1:]:
        level = level * one(*cut)
    return level


def normal_values(key, dims, spread, reach, pieces=(), kind=jnp.bfloat16):
    result = spread * jax.random.normal(key, dims, jnp.float32)
    if pieces:
        result = result * steps_of(key, dims, pieces, -0.22, 0.18)
    return jnp.clip(result, -reach, reach).astype(kind)


def setup_inputs(seed: int = 0) -> dict:
    key_list = jax.random.split(jax.random.key(seed), 6)
    charges = normal_values(key_list[0], (PARTICLES,), 2.0, 12.0, ((0, 32),), jnp.float32)
    cells = plant(jax.random.randint(key_list[1], (SPREAD, PARTICLES), 0, ZDEV * NX * NY), jax.random.fold_in(key_list[1], 1), 0, (ZDEV * NX * NY) - 1).astype(jnp.int32)
    splines = jnp.clip(0.05 + 0.95 * jax.random.uniform(key_list[2], (SPREAD, PARTICLES), jnp.float32) ** steps_of(key_list[2], (SPREAD, PARTICLES), ((1, 32),), -0.2, 0.2), 0.05, 1.0)
    counts = draw_counts(jax.random.fold_in(key_list[5], 71), 0)
    green = normal_values(key_list[4], (NX, KYB, NZ, NZ), NZ ** -0.5, 0.3125, ((0, 32),))
    return {"charges": charges, "cells": cells, "splines": splines, "counts": counts, "green": green}


def reference(charges, cells, splines, counts, green):
    devices = N_ZG * N_XY
    slab = NZ // devices
    slots = jnp.arange(devices * PART_DEV, dtype=jnp.int32)
    owner = slots // PART_DEV
    rank = slots - owner * PART_DEV
    live = (rank < counts[owner]).astype(jnp.float32)
    values = splines * (charges * live)[None, :]
    offsets = cells + (owner * (slab * NX * NY))[None, :]
    density = jnp.zeros((NZ * NX * NY,), jnp.float32).at[offsets.reshape(-1)].add(values.reshape(-1))
    density = density.reshape(NZ, NX, NY)
    norm = jnp.sqrt(jnp.float32(NX * NY))
    transformed = jnp.fft.fft2(density, axes=(1, 2)) / norm
    spectrum = jnp.stack([jnp.real(transformed), jnp.imag(transformed)], axis=1).astype(jnp.bfloat16)

    def one_column(pair):
        matrices, plane = pair
        blocks = plane.astype(jnp.float32).reshape(NZ, 2, KYB, NY // KYB)
        mixed = jnp.einsum('bzw,wcbj->zcbj', matrices.astype(jnp.float32), blocks)
        return mixed.reshape(NZ, 2, NY).astype(jnp.bfloat16)
    columns = lax.map(one_column, (green, jnp.moveaxis(spectrum, 2, 0)))
    mixed = jnp.moveaxis(columns, 0, 2).astype(jnp.float32)
    complex_hat = lax.complex(mixed[:, 0], mixed[:, 1])
    potential = jnp.real(jnp.fft.ifft2(complex_hat, axes=(1, 2))) * norm
    return potential.astype(jnp.float32)
```

```python
import functools
import math

import jax
import jax.numpy as jnp
import numpy as np
from jax import lax
from jax.experimental import pallas as pl
from jax.experimental.pallas import tpu as pltpu
from jax.sharding import PartitionSpec as P


F32 = jnp.float32
BF16 = jnp.bfloat16
LANES = 128
POINTS = 512
SIDE = 256
VMEM = 60 * 2**20
AXES = ("zg", "xy")


def round_up(value, to):
    return -(-value // to) * to


def split(value):
    high = value.astype(BF16)
    return high, (value - high.astype(F32)).astype(BF16)


def dot(left, right):
    return jnp.dot(left, right, preferred_element_type=F32)


def table(length, block):
    index = np.arange(length)
    angle = (index[:, None] * index[None, :] % length) * (2.0 * math.pi / length)
    blocks = np.stack(
        [np.cos(angle).reshape(length, -1, block), np.sin(angle).reshape(length, -1, block)], axis=2
    ).reshape(length, -1)
    high = blocks.astype(np.float32).astype(BF16)
    low = (blocks - high.astype(np.float64)).astype(np.float32).astype(BF16)
    return high, low


def density_kernel(starts, cells, values, high_ref, low_ref, total):
    who, plane = pl.program_id(0), pl.program_id(1)
    buckets, _, side = total.shape
    rows = high_ref.shape[1] // buckets
    width = side // rows
    names = lax.broadcasted_iota(jnp.int32, (side, POINTS), 0)

    def product(bucket, piece):
        lines = range(POINTS // LANES)
        cell = jnp.concatenate([cells[0, pl.ds(piece + k, 1), :] for k in lines], axis=1)
        value = jnp.concatenate([values[0, pl.ds(piece + k, 1), :] for k in lines], axis=1)
        cell = cell - bucket * (side * side)
        inside = (cell >= 0) & (cell < side * side)
        row = cell // side
        row = (row % width) * rows + row // width
        hit = names == jnp.where(inside, row, -1)
        high = value.astype(BF16).astype(F32)
        low = value - high
        left = jnp.concatenate(
            [jnp.where(hit, high, 0.0).astype(BF16), jnp.where(hit, low, 0.0).astype(BF16)], axis=0
        )
        right = jnp.where(names == (cell & (side - 1)), 1.0, 0.0).astype(BF16)
        return lax.dot_general(left, right, (((1,), (1,)), ((), ())), preferred_element_type=F32)

    for k in range(buckets):
        total[k] = product(plane * buckets + k, starts[who, plane * buckets + k] // LANES)
    for k in range(buckets):
        bucket = plane * buckets + k
        start = starts[who, bucket] // LANES

        def step(turn, carry, k=k, bucket=bucket, start=start):
            total[k] += product(bucket, start + turn * (POINTS // LANES))
            return carry

        lax.fori_loop(1, (starts[who, bucket + 1] - start * LANES + POINTS - 1) // POINTS, step, 0)
    for k in range(buckets):
        block = total[k, :side, :] + total[k, side:, :]
        for part in range(width):
            high, low = split(block[part * rows:(part + 1) * rows, :])
            place = (0, slice(k * rows, (k + 1) * rows), slice(part * side, (part + 1) * side))
            high_ref[place] = high
            low_ref[place] = low


def make_density(starts, cells, values, slab, nx, ny):
    side = SIDE
    buckets = nx * ny // (side * side)
    spec = pl.BlockSpec((1,) + cells.shape[1:], lambda w, z, s: (w, 0, 0))
    out = pl.BlockSpec((1, nx, ny), lambda w, z, s: (w * slab + z, 0, 0))
    shape = jax.ShapeDtypeStruct((2 * slab, nx, ny), BF16)
    return pl.pallas_call(
        density_kernel,
        out_shape=(shape, shape),
        grid_spec=pltpu.PrefetchScalarGridSpec(
            num_scalar_prefetch=1,
            grid=(2, slab),
            in_specs=[spec, spec],
            out_specs=(out, out),
            scratch_shapes=[pltpu.VMEM((buckets, 2 * side, side), F32)],
        ),
        cost_estimate=pl.CostEstimate(
            flops=2 * slab * buckets * 4 * side * side * POINTS, bytes_accessed=8 * slab * nx * ny, transcendentals=0
        ),
        compiler_params=pltpu.CompilerParams(vmem_limit_bytes=VMEM),
        name="density",
    )(starts, cells, values)


def forward_kernel(places, scale, high_ref, low_ref, y_table, x_table, out_ref, real, imag):
    turn = pl.program_id(0)
    planes = high_ref.shape[0]
    stride = out_ref.shape[2]
    half = x_table.shape[0] // 2
    pieces = []
    for k in range(planes):
        left = jnp.concatenate([high_ref[k], low_ref[k], high_ref[k]], axis=1)
        high, low = split(dot(left, y_table[...]))
        pieces.append(jnp.concatenate([high, low, high], axis=0))
    both = dot(x_table[...], jnp.concatenate(pieces, axis=1)) * scale
    for k in range(planes):
        cut = both[:, k * 2 * LANES:(k + 1) * 2 * LANES]
        rows = pl.ds(places[turn * planes + k], half, stride=stride)
        real[rows, :] = cut[:half, :LANES] - cut[half:, LANES:]
        imag[rows, :] = -(cut[:half, LANES:] + cut[half:, :LANES])

    @pl.when(turn == pl.num_programs(0) - 1)
    def _():
        owners, waves = out_ref.shape[0], out_ref.shape[1]
        count = waves * stride

        def step(owner, carry):
            rows = pl.ds(pl.multiple_of(owner * count, 8), count)
            out_ref[owner, :, :, :LANES] = real[rows, :].reshape(waves, stride, LANES).astype(BF16)
            out_ref[owner, :, :, LANES:] = imag[rows, :].reshape(waves, stride, LANES).astype(BF16)
            return carry

        lax.fori_loop(0, owners, step, 0)


def make_forward(places, density, y_table, x_table, block, owners, waves, stride, scale):
    planes, nx, ny = density[0].shape
    half = owners * waves
    plane = pl.BlockSpec((2, nx, ny), lambda p, s: (p, 0, 0))
    shape = (owners, waves, stride, 2 * LANES)
    return pl.pallas_call(
        lambda places, *refs: forward_kernel(places, scale, *refs),
        out_shape=jax.ShapeDtypeStruct(shape, BF16),
        grid_spec=pltpu.PrefetchScalarGridSpec(
            num_scalar_prefetch=1,
            grid=(planes // 2,),
            in_specs=[
                plane,
                plane,
                pl.BlockSpec((3 * ny, 2 * LANES), lambda p, s: (0, block)),
                pl.BlockSpec(x_table.shape, lambda p, s: (0, 0)),
            ],
            out_specs=pl.BlockSpec(shape, lambda p, s: (0, 0, 0, 0)),
            scratch_shapes=[pltpu.VMEM((half * stride, LANES), F32)] * 2,
        ),
        cost_estimate=pl.CostEstimate(
            flops=2 * planes * 3 * 2 * nx * ny * 2 * LANES, bytes_accessed=4 * planes * nx * ny, transcendentals=0
        ),
        compiler_params=pltpu.CompilerParams(vmem_limit_bytes=VMEM),
        name="forward",
    )(places, *density, y_table, x_table)


def mix_kernel(green_ref, seen_ref, order_ref, out_ref, real, imag):
    mix(dot(green_ref[0, 0], arranged(order_ref, seen_ref).astype(BF16)), out_ref, real, imag)


def arranged(order_ref, seen_ref):
    seen = seen_ref[:, 0, :, :].astype(F32)
    seen = seen.reshape(seen.shape[0] * seen.shape[1], seen.shape[2]).astype(BF16)
    return dot(order_ref[...], seen)


def mix(mixed, out_ref, real, imag):
    turn = pl.program_id(0)
    groups, planes, waves, _ = out_ref.shape
    depth = groups * planes
    stride = real.shape[0] // depth
    rows = pl.ds(turn, depth, stride=stride)
    real[rows, :] = mixed[:, :LANES]
    imag[rows, :] = mixed[:, LANES:]

    @pl.when(turn == pl.num_programs(0) - 1)
    def _():
        def step(group, carry):
            for plane in range(planes):
                rows = pl.ds(pl.multiple_of((group * planes + plane) * stride, 8), waves)
                out_ref[group, plane, :, :LANES] = real[rows, :].astype(BF16)
                out_ref[group, plane, :, LANES:] = imag[rows, :].astype(BF16)
            return carry

        lax.fori_loop(0, groups, step, 0)


def mix_block(green, seen, order, block, devices, slab):
    waves, _, depth, _ = green.shape
    groups, _, rows, width = seen.shape
    padded = round_up(waves, 8)
    shape = (devices, slab, padded, width)
    stride = padded if padded % 16 else padded + 8
    return pl.pallas_call(
        mix_kernel,
        out_shape=jax.ShapeDtypeStruct(shape, BF16),
        grid=(waves,),
        in_specs=[
            pl.BlockSpec((1, 1, depth, depth), lambda u: (u, block, 0, 0)),
            pl.BlockSpec((groups, 1, rows, width), lambda u: (0, u, 0, 0)),
            pl.BlockSpec(order.shape, lambda u: (0, 0)),
        ],
        out_specs=pl.BlockSpec(shape, lambda u: (0, 0, 0, 0)),
        scratch_shapes=[pltpu.VMEM((depth * stride, LANES), F32)] * 2,
        cost_estimate=pl.CostEstimate(
            flops=waves * 4 * depth * depth * width,
            bytes_accessed=2 * waves * depth * (depth + 2 * width), transcendentals=0,
        ),
        compiler_params=pltpu.CompilerParams(vmem_limit_bytes=VMEM),
        name="mix",
    )(green, seen, order)


def after(value, other):
    return pl.pallas_call(
        lambda value_ref, other_ref, out_ref: None,
        out_shape=jax.ShapeDtypeStruct(value.shape, value.dtype),
        in_specs=[pl.BlockSpec(memory_space=pl.ANY)] * 2,
        out_specs=pl.BlockSpec(memory_space=pl.ANY),
        input_output_aliases={0: 0},
        name="after",
    )(value, other)


def inverse_kernel(scale, first, *refs):
    if first:
        seen_ref, x_table, y_table, out_ref = refs
    else:
        seen_ref, x_table, y_table, so_far, out_ref = refs
    value = seen_ref[:, 0, :, :]
    both = dot(x_table[...], value.reshape(value.shape[0] * value.shape[1], value.shape[2]))
    nx = both.shape[0] // 2
    real = both[:nx, :LANES] - both[nx:, LANES:]
    imag = -(both[:nx, LANES:] + both[nx:, :LANES])
    middle = (jnp.concatenate([real, imag], axis=1) * scale).astype(BF16)
    result = dot(middle, y_table[0])
    if not first:
        result += so_far[0]
    out_ref[0] = result


def make_inverse(seen, x_table, y_table, block, so_far, scale):
    devices, slab, padded, width = seen.shape
    nx = x_table.shape[0] // 2
    ny = y_table.shape[2]
    out = pl.BlockSpec((1, nx, ny), lambda p: (p, 0, 0))
    first = so_far is None
    return pl.pallas_call(
        functools.partial(inverse_kernel, scale, first),
        out_shape=jax.ShapeDtypeStruct((slab, nx, ny), F32),
        grid=(slab,),
        in_specs=[
            pl.BlockSpec((devices, 1, padded, width), lambda p: (0, p, 0, 0)),
            pl.BlockSpec(x_table.shape, lambda p: (0, 0)),
            pl.BlockSpec((1, 2 * LANES, ny), lambda p: (block, 0, 0)),
        ]
        + ([] if first else [out]),
        out_specs=out,
        input_output_aliases={} if first else {3: 0},
        cost_estimate=pl.CostEstimate(
            flops=2 * slab * nx * width * (2 * nx + ny), bytes_accessed=8 * slab * nx * ny, transcendentals=0
        ),
        compiler_params=pltpu.CompilerParams(vmem_limit_bytes=VMEM),
        name="inverse",
    )(seen, x_table, y_table, *([] if first else [so_far]))


def shards(nx, ny, charges, cells, splines, counts, green):
    n_zg, n_xy = lax.axis_size("zg"), lax.axis_size("xy")
    devices = n_zg * n_xy
    inner = n_xy // 2
    owners = devices // 2
    depth = green.shape[2]
    blocks = green.shape[1]
    slab = depth // devices
    waves = nx // devices
    stride = round_up(2 * slab, 8)
    padded = round_up(waves, 8)
    side = lax.axis_index("xy") // inner
    swap = [(i, (i + inner) % n_xy) for i in range(n_xy)]
    groups = [
        [g * n_xy + s * inner + r for g in range(n_zg) for r in range(inner)] for s in range(2)
    ]
    scale = 1.0 / math.sqrt(nx * ny)

    slots = charges.shape[0]
    live = (jnp.arange(slots, dtype=jnp.int32) < counts[0]).astype(F32)
    values = splines * (charges * live)[None, :]
    sorted_cells, sorted_values = lax.sort((cells.reshape(-1), values.reshape(-1)), num_keys=1, is_stable=False)
    other_cells = lax.ppermute(sorted_cells, "xy", swap)
    other_values = lax.ppermute(sorted_values, "xy", swap)
    both_cells = jnp.where(
        side == 0, jnp.stack([sorted_cells, other_cells]), jnp.stack([other_cells, sorted_cells])
    )
    both_values = jnp.where(
        side == 0, jnp.stack([sorted_values, other_values]), jnp.stack([other_values, sorted_values])
    )
    size = SIDE * SIDE
    edges = jnp.arange(slab * nx * ny // size + 1, dtype=jnp.int32) * size
    starts = jnp.sum((both_cells[:, None, :] < edges[None, :, None]).astype(jnp.int32), axis=2)
    both_cells = jnp.pad(both_cells, ((0, 0), (0, POINTS)), constant_values=-1)
    both_values = jnp.pad(both_values, ((0, 0), (0, POINTS)))
    density = make_density(starts, both_cells.reshape(2, -1, LANES), both_values.reshape(2, -1, LANES), slab, nx, ny)

    high, low = table(ny, LANES)
    y_high, y_low = jnp.asarray(high), jnp.asarray(low)

    def trig(name):
        parts = name.reshape(ny, blocks, 2, LANES)
        return parts[:, :, 0, :].reshape(ny, ny), parts[:, :, 1, :].reshape(ny, ny)

    cos_high, sin_high = trig(y_high)
    cos_low, sin_low = trig(y_low)

    def rows_of(value, half):
        value = value.reshape(n_zg, 2, inner * waves, nx)
        return lax.dynamic_index_in_dim(value, half, 1, keepdims=False).reshape(owners * waves, nx)

    x_high = jnp.concatenate([rows_of(cos_high, side), rows_of(sin_high, side)])
    x_low = jnp.concatenate([rows_of(cos_low, side), rows_of(sin_low, side)])
    x_forward = jnp.concatenate([x_high, x_high, x_low], axis=1)
    y_forward = jnp.concatenate([y_high, y_high, y_low], axis=0)

    def inverse_table(value):
        value = jnp.pad(value.reshape(nx, devices, waves), ((0, 0), (0, 0), (0, padded - waves)))
        return value.reshape(nx, devices * padded)

    x_inverse = jnp.concatenate([inverse_table(cos_high), inverse_table(sin_high)])
    y_inverse = jnp.concatenate(
        [cos_high.reshape(blocks, LANES, ny), sin_high.reshape(blocks, LANES, ny)], axis=1
    )

    place = np.full((n_zg, inner, stride), -1)
    for half in range(2):
        ids = (np.arange(n_zg)[:, None] * 2 + half) * inner + np.arange(inner)[None, :]
        place[:, :, half * slab:(half + 1) * slab] = ids[:, :, None] * slab + np.arange(slab)
    order = (jnp.arange(depth)[:, None] == jnp.asarray(place.reshape(-1))[None, :]).astype(BF16)

    places = jnp.arange(2 * slab, dtype=jnp.int32)

    def exchange(value):
        return lax.all_to_all(
            value, AXES, split_axis=0, concat_axis=0, tiled=True, axis_index_groups=groups
        )

    result = None
    seen = []
    for b in range(blocks):
        value = make_forward(places, density, y_forward, x_forward, b, owners, waves, stride, scale)
        seen.append(exchange(value))
    for b in range(blocks):
        value = mix_block(green, seen[b], order, b, devices, slab)
        if b == 0:
            together = lax.psum(seen[-1][:1, :1, :1, :LANES].astype(F32), AXES)
            value = after(value, together)
        value = lax.all_to_all(value, AXES, split_axis=0, concat_axis=0, tiled=True)
        result = make_inverse(value, x_inverse, y_inverse, b, result, scale)
    return result


def solution(mesh):
    in_specs = (
        P(AXES),
        P(None, AXES),
        P(None, AXES),
        P(AXES),
        P(AXES, None, None, None),
    )
    out_specs = P(AXES, None, None)

    def step(charges, cells, splines, counts, green):
        nx = green.shape[0]
        ny = green.shape[1] * LANES

        def body(*operands):
            return shards(nx, ny, *operands)

        return jax.shard_map(body, mesh=mesh, in_specs=in_specs, out_specs=out_specs, check_vma=False)(
            charges, cells, splines, counts, green
        )

    return step
```

```python
import functools
import math

import jax
import jax.numpy as jnp
import numpy as np
from jax import lax
from jax.experimental import pallas as pl
from jax.experimental.pallas import tpu as pltpu
from jax.sharding import PartitionSpec as P


F32 = jnp.float32
BF16 = jnp.bfloat16
LANES = 128
POINTS = 512
SIDE = 256
VMEM = 66_000_000
AXES = ("zg", "xy")


def round_up(value, to):
    return -(-value // to) * to


def split(value):
    high = value.astype(BF16)
    return high, (value - high.astype(F32)).astype(BF16)


def dot(left, right):
    return jnp.dot(left, right, preferred_element_type=F32)


def table(length, block):
    index = np.arange(length)
    angle = (index[:, None] * index[None, :] % length) * (2.0 * math.pi / length)
    blocks = np.stack(
        [np.cos(angle).reshape(length, -1, block), np.sin(angle).reshape(length, -1, block)], axis=2
    ).reshape(length, -1)
    high = blocks.astype(np.float32).astype(BF16)
    low = (blocks - high.astype(np.float64)).astype(np.float32).astype(BF16)
    return high, low


def density_kernel(starts, cells, values, high_ref, low_ref, total):
    who, plane = pl.program_id(0), pl.program_id(1)
    buckets, _, side = total.shape
    rows = high_ref.shape[1] // buckets
    width = side // rows
    names = lax.broadcasted_iota(jnp.int32, (side, POINTS), 0)

    def product(bucket, piece):
        lines = range(POINTS // LANES)
        cell = jnp.concatenate([cells[0, pl.ds(piece + k, 1), :] for k in lines], axis=1)
        value = jnp.concatenate([values[0, pl.ds(piece + k, 1), :] for k in lines], axis=1)
        cell = cell - bucket * (side * side)
        inside = (cell >= 0) & (cell < side * side)
        row = cell // side
        row = (row % width) * rows + row // width
        hit = names == jnp.where(inside, row, -1)
        high = value.astype(BF16).astype(F32)
        low = value - high
        left = jnp.concatenate(
            [jnp.where(hit, high, 0.0).astype(BF16), jnp.where(hit, low, 0.0).astype(BF16)], axis=0
        )
        right = jnp.where(names == (cell & (side - 1)), 1.0, 0.0).astype(BF16)
        return lax.dot_general(left, right, (((1,), (1,)), ((), ())), preferred_element_type=F32)

    for k in range(buckets):
        total[k] = product(plane * buckets + k, starts[who, plane * buckets + k] // LANES)
    for k in range(buckets):
        bucket = plane * buckets + k
        start = starts[who, bucket] // LANES

        def step(turn, carry, k=k, bucket=bucket, start=start):
            total[k] += product(bucket, start + turn * (POINTS // LANES))
            return carry

        lax.fori_loop(1, (starts[who, bucket + 1] - start * LANES + POINTS - 1) // POINTS, step, 0)
    for k in range(buckets):
        block = total[k, :side, :] + total[k, side:, :]
        for part in range(width):
            high, low = split(block[part * rows:(part + 1) * rows, :])
            place = (0, slice(k * rows, (k + 1) * rows), slice(part * side, (part + 1) * side))
            high_ref[place] = high
            low_ref[place] = low


def make_density(starts, cells, values, slab, nx, ny):
    side = SIDE
    buckets = nx * ny // (side * side)
    spec = pl.BlockSpec((1,) + cells.shape[1:], lambda w, z, s: (w, 0, 0))
    out = pl.BlockSpec((1, nx, ny), lambda w, z, s: (w * slab + z, 0, 0))
    shape = jax.ShapeDtypeStruct((2 * slab, nx, ny), BF16)
    return pl.pallas_call(
        density_kernel,
        out_shape=(shape, shape),
        grid_spec=pltpu.PrefetchScalarGridSpec(
            num_scalar_prefetch=1,
            grid=(2, slab),
            in_specs=[spec, spec],
            out_specs=(out, out),
            scratch_shapes=[pltpu.VMEM((buckets, 2 * side, side), F32)],
        ),
        cost_estimate=pl.CostEstimate(
            flops=2 * slab * buckets * 4 * side * side * POINTS, bytes_accessed=8 * slab * nx * ny, transcendentals=0
        ),
        compiler_params=pltpu.CompilerParams(vmem_limit_bytes=VMEM),
        name="density",
    )(starts, cells, values)


def forward_kernel(places, scale, high_ref, low_ref, y_table, x_table, out_ref, real, imag):
    turn = pl.program_id(0)
    planes = high_ref.shape[0]
    stride = out_ref.shape[2]
    half = x_table.shape[0] // 2
    pieces = []
    for k in range(planes):
        left = jnp.concatenate([high_ref[k], low_ref[k], high_ref[k]], axis=1)
        high, low = split(dot(left, y_table[...]))
        pieces.append(jnp.concatenate([high, low, high], axis=0))
    both = dot(x_table[...], jnp.concatenate(pieces, axis=1)) * scale
    for k in range(planes):
        cut = both[:, k * 2 * LANES:(k + 1) * 2 * LANES]
        rows = pl.ds(places[turn * planes + k], half, stride=stride)
        real[rows, :] = cut[:half, :LANES] - cut[half:, LANES:]
        imag[rows, :] = -(cut[:half, LANES:] + cut[half:, :LANES])

    @pl.when(turn == pl.num_programs(0) - 1)
    def _():
        owners, waves = out_ref.shape[0], out_ref.shape[1]
        count = waves * stride

        def step(owner, carry):
            rows = pl.ds(pl.multiple_of(owner * count, 8), count)
            out_ref[owner, :, :, :LANES] = real[rows, :].reshape(waves, stride, LANES).astype(BF16)
            out_ref[owner, :, :, LANES:] = imag[rows, :].reshape(waves, stride, LANES).astype(BF16)
            return carry

        lax.fori_loop(0, owners, step, 0)


def make_forward(places, density, y_table, x_table, block, owners, waves, stride, scale):
    planes, nx, ny = density[0].shape
    half = owners * waves
    plane = pl.BlockSpec((2, nx, ny), lambda p, s: (p, 0, 0))
    shape = (owners, waves, stride, 2 * LANES)
    return pl.pallas_call(
        lambda places, *refs: forward_kernel(places, scale, *refs),
        out_shape=jax.ShapeDtypeStruct(shape, BF16),
        grid_spec=pltpu.PrefetchScalarGridSpec(
            num_scalar_prefetch=1,
            grid=(planes // 2,),
            in_specs=[
                plane,
                plane,
                pl.BlockSpec((3 * ny, 2 * LANES), lambda p, s: (0, block)),
                pl.BlockSpec(x_table.shape, lambda p, s: (0, 0)),
            ],
            out_specs=pl.BlockSpec(shape, lambda p, s: (0, 0, 0, 0)),
            scratch_shapes=[pltpu.VMEM((half * stride, LANES), F32)] * 2,
        ),
        cost_estimate=pl.CostEstimate(
            flops=2 * planes * 3 * 2 * nx * ny * 2 * LANES, bytes_accessed=4 * planes * nx * ny, transcendentals=0
        ),
        compiler_params=pltpu.CompilerParams(vmem_limit_bytes=VMEM),
        name="forward",
    )(places, *density, y_table, x_table)


def mix_kernel(green_ref, seen_ref, order_ref, out_ref, real, imag):
    mix(dot(green_ref[0, 0], arranged(order_ref, seen_ref).astype(BF16)), out_ref, real, imag)


def arranged(order_ref, seen_ref):
    seen = seen_ref[:, 0, :, :].astype(F32)
    seen = seen.reshape(seen.shape[0] * seen.shape[1], seen.shape[2]).astype(BF16)
    return dot(order_ref[...], seen)


def mix(mixed, out_ref, real, imag):
    turn = pl.program_id(0)
    groups, planes, waves, _ = out_ref.shape
    depth = groups * planes
    stride = real.shape[0] // depth
    rows = pl.ds(turn, depth, stride=stride)
    real[rows, :] = mixed[:, :LANES]
    imag[rows, :] = mixed[:, LANES:]

    @pl.when(turn == pl.num_programs(0) - 1)
    def _():
        def step(group, carry):
            for plane in range(planes):
                rows = pl.ds(pl.multiple_of((group * planes + plane) * stride, 8), waves)
                out_ref[group, plane, :, :LANES] = real[rows, :].astype(BF16)
                out_ref[group, plane, :, LANES:] = imag[rows, :].astype(BF16)
            return carry

        lax.fori_loop(0, groups, step, 0)


def mix_block(green, seen, order, block, devices, slab):
    waves, _, depth, _ = green.shape
    groups, _, rows, width = seen.shape
    padded = round_up(waves, 8)
    shape = (devices, slab, padded, width)
    stride = padded if padded % 16 else padded + 8
    return pl.pallas_call(
        mix_kernel,
        out_shape=jax.ShapeDtypeStruct(shape, BF16),
        grid=(waves,),
        in_specs=[
            pl.BlockSpec((1, 1, depth, depth), lambda u: (u, block, 0, 0)),
            pl.BlockSpec((groups, 1, rows, width), lambda u: (0, u, 0, 0)),
            pl.BlockSpec(order.shape, lambda u: (0, 0)),
        ],
        out_specs=pl.BlockSpec(shape, lambda u: (0, 0, 0, 0)),
        scratch_shapes=[pltpu.VMEM((depth * stride, LANES), F32)] * 2,
        cost_estimate=pl.CostEstimate(
            flops=waves * 4 * depth * depth * width,
            bytes_accessed=2 * waves * depth * (depth + 2 * width), transcendentals=0,
        ),
        compiler_params=pltpu.CompilerParams(vmem_limit_bytes=VMEM),
        name="mix",
    )(green, seen, order)


def inverse_kernel(scale, first, *refs):
    if first:
        seen_ref, x_table, y_table, out_ref = refs
    else:
        seen_ref, x_table, y_table, so_far, out_ref = refs
    value = seen_ref[:, 0, :, :]
    both = dot(x_table[...], value.reshape(value.shape[0] * value.shape[1], value.shape[2]))
    nx = both.shape[0] // 2
    real = both[:nx, :LANES] - both[nx:, LANES:]
    imag = -(both[:nx, LANES:] + both[nx:, :LANES])
    middle = (jnp.concatenate([real, imag], axis=1) * scale).astype(BF16)
    result = dot(middle, y_table[0])
    if not first:
        result += so_far[0]
    out_ref[0] = result


def make_inverse(seen, x_table, y_table, block, so_far, scale):
    devices, slab, padded, width = seen.shape
    nx = x_table.shape[0] // 2
    ny = y_table.shape[2]
    out = pl.BlockSpec((1, nx, ny), lambda p: (p, 0, 0))
    first = so_far is None
    return pl.pallas_call(
        functools.partial(inverse_kernel, scale, first),
        out_shape=jax.ShapeDtypeStruct((slab, nx, ny), F32),
        grid=(slab,),
        in_specs=[
            pl.BlockSpec((devices, 1, padded, width), lambda p: (0, p, 0, 0)),
            pl.BlockSpec(x_table.shape, lambda p: (0, 0)),
            pl.BlockSpec((1, 2 * LANES, ny), lambda p: (block, 0, 0)),
        ]
        + ([] if first else [out]),
        out_specs=out,
        input_output_aliases={} if first else {3: 0},
        cost_estimate=pl.CostEstimate(
            flops=2 * slab * nx * width * (2 * nx + ny), bytes_accessed=8 * slab * nx * ny, transcendentals=0
        ),
        compiler_params=pltpu.CompilerParams(vmem_limit_bytes=VMEM),
        name="inverse",
    )(seen, x_table, y_table, *([] if first else [so_far]))


def shards(nx, ny, charges, cells, splines, counts, green):
    n_zg, n_xy = lax.axis_size("zg"), lax.axis_size("xy")
    devices = n_zg * n_xy
    inner = n_xy // 2
    owners = devices // 2
    depth = green.shape[2]
    blocks = green.shape[1]
    slab = depth // devices
    waves = nx // devices
    stride = round_up(2 * slab, 8)
    padded = round_up(waves, 8)
    side = lax.axis_index("xy") // inner
    swap = [(i, (i + inner) % n_xy) for i in range(n_xy)]
    groups = [
        [g * n_xy + s * inner + r for g in range(n_zg) for r in range(inner)] for s in range(2)
    ]
    scale = 1.0 / math.sqrt(nx * ny)

    slots = charges.shape[0]
    live = (jnp.arange(slots, dtype=jnp.int32) < counts[0]).astype(F32)
    values = splines * (charges * live)[None, :]
    sorted_cells, sorted_values = lax.sort((cells.reshape(-1), values.reshape(-1)), num_keys=1, is_stable=False)
    other_cells = lax.ppermute(sorted_cells, "xy", swap)
    other_values = lax.ppermute(sorted_values, "xy", swap)
    both_cells = jnp.where(
        side == 0, jnp.stack([sorted_cells, other_cells]), jnp.stack([other_cells, sorted_cells])
    )
    both_values = jnp.where(
        side == 0, jnp.stack([sorted_values, other_values]), jnp.stack([other_values, sorted_values])
    )
    size = SIDE * SIDE
    edges = jnp.arange(slab * nx * ny // size + 1, dtype=jnp.int32) * size
    starts = jnp.sum((both_cells[:, None, :] < edges[None, :, None]).astype(jnp.int32), axis=2)
    both_cells = jnp.pad(both_cells, ((0, 0), (0, POINTS)), constant_values=-1)
    both_values = jnp.pad(both_values, ((0, 0), (0, POINTS)))
    density = make_density(starts, both_cells.reshape(2, -1, LANES), both_values.reshape(2, -1, LANES), slab, nx, ny)

    high, low = table(ny, LANES)
    y_high, y_low = jnp.asarray(high), jnp.asarray(low)

    def trig(name):
        parts = name.reshape(ny, blocks, 2, LANES)
        return parts[:, :, 0, :].reshape(ny, ny), parts[:, :, 1, :].reshape(ny, ny)

    cos_high, sin_high = trig(y_high)
    cos_low, sin_low = trig(y_low)

    def rows_of(value, half):
        value = value.reshape(n_zg, 2, inner * waves, nx)
        return lax.dynamic_index_in_dim(value, half, 1, keepdims=False).reshape(owners * waves, nx)

    x_high = jnp.concatenate([rows_of(cos_high, side), rows_of(sin_high, side)])
    x_low = jnp.concatenate([rows_of(cos_low, side), rows_of(sin_low, side)])
    x_forward = jnp.concatenate([x_high, x_high, x_low], axis=1)
    y_forward = jnp.concatenate([y_high, y_high, y_low], axis=0)

    def inverse_table(value):
        value = jnp.pad(value.reshape(nx, devices, waves), ((0, 0), (0, 0), (0, padded - waves)))
        return value.reshape(nx, devices * padded)

    x_inverse = jnp.concatenate([inverse_table(cos_high), inverse_table(sin_high)])
    y_inverse = jnp.concatenate(
        [cos_high.reshape(blocks, LANES, ny), sin_high.reshape(blocks, LANES, ny)], axis=1
    )

    place = np.full((n_zg, inner, stride), -1)
    for half in range(2):
        ids = (np.arange(n_zg)[:, None] * 2 + half) * inner + np.arange(inner)[None, :]
        place[:, :, half * slab:(half + 1) * slab] = ids[:, :, None] * slab + np.arange(slab)
    order = (jnp.arange(depth)[:, None] == jnp.asarray(place.reshape(-1))[None, :]).astype(BF16)

    places = jnp.arange(2 * slab, dtype=jnp.int32)

    def exchange(value):
        return lax.all_to_all(
            value, AXES, split_axis=0, concat_axis=0, tiled=True, axis_index_groups=groups
        )

    result = None
    seen = []
    for b in range(blocks):
        value = make_forward(places, density, y_forward, x_forward, b, owners, waves, stride, scale)
        seen.append(exchange(value))
    for b in range(blocks):
        value = mix_block(green, seen[b], order, b, devices, slab)
        value = lax.all_to_all(value, AXES, split_axis=0, concat_axis=0, tiled=True)
        result = make_inverse(value, x_inverse, y_inverse, b, result, scale)
    return result


def solution(mesh):
    in_specs = (
        P(AXES),
        P(None, AXES),
        P(None, AXES),
        P(AXES),
        P(AXES, None, None, None),
    )
    out_specs = P(AXES, None, None)

    def step(charges, cells, splines, counts, green):
        nx = green.shape[0]
        ny = green.shape[1] * LANES

        def body(*operands):
            return shards(nx, ny, *operands)

        return jax.shard_map(body, mesh=mesh, in_specs=in_specs, out_specs=out_specs, check_vma=False)(
            charges, cells, splines, counts, green
        )

    return step
```
